32 devices in a mesh: gx: 16 (over z, y, x), gy: 2 (over core).
Axes of the slice: x: 2, y: 2, z: 4, core: 2. Of those that a mesh axis runs over, the one named last changes fastest.
Arguments:
- history: bfloat16 [128, 2048, 256], P(('gx', 'gy')), may hold values from -100 to 100
- lengths: int32 [128], P(('gx', 'gy')), may hold values from 16 to 2048
- candidates: int32 [128, 64], P(('gx', 'gy')), may hold values from 0 to 131071, as said below
- item_table: bfloat16 [131072, 512], P(('gx', 'gy')), may hold values from -6 to 6
- value_weight: bfloat16 [256, 256], replicated, may hold values from -0.375 to 0.375
- click_hidden: bfloat16 [768, 256], replicated, may hold values from -0.21875 to 0.21875
- convert_hidden: bfloat16 [768, 256], replicated, may hold values from -0.21875 to 0.21875
- click_output: bfloat16 [256], replicated, may hold values from -0.75 to 0.75
- convert_output: bfloat16 [256], replicated, may hold values from -0.75 to 0.75
Outputs:
- click_rate: float32 [128, 64], P(('gx', 'gy'))
- click_conversion: float32 [128, 64], P(('gx', 'gy'))
The draws below stay inside these ranges and needn't reach their ends.
Inputs may be any that keep to these rules, and one draw needn't show every extreme that they name: Device k holds the table rows k * 4096 to (k + 1) * 4096 - 1. Of the 256 candidates of one device, at most 16 are items of one device's rows, and exactly 16 are items of some device's rows.
All inputs are finite; a program needn't handle non-finite values.
Results may differ from the reference program's by a relative error of at most 0.0028.
Values may be sent and summed in bfloat16 or wider, within the bound.
A program may use at most 64 MiB of HBM per device.

```python
import math
import jax
import jax.numpy as jnp
from jax import lax

D = 256
HEADS = 4
HEAD_DIM = 64
BLK = 128
MAXB = 16
U_DEV = 4
CAND = 64
ITEM_DEV = 4096
TH = 256
USERS = 128
ITEMS = 131072
CAP = 16
DEVICES = 32


def pick_candidates(key):
    impressions = U_DEV * CAND
    slot_total = DEVICES * CAP

    def per_device(device_key):
        key_order, key_full, key_shuffle, key_row = jax.random.split(device_key, 4)
        visit = jax.random.permutation(key_order, slot_total)
        ranking = jnp.zeros((slot_total,), jnp.int32).at[visit].set(jnp.arange(slot_total, dtype=jnp.int32))
        full_owner = jax.random.randint(key_full, (), 0, DEVICES)
        slot_owner = jnp.arange(slot_total, dtype=jnp.int32) // CAP
        priority = ranking - jnp.where(slot_owner == full_owner, slot_total, 0)
        chosen = jnp.argsort(priority)[:impressions].astype(jnp.int32)
        chosen = jax.random.permutation(key_shuffle, chosen)
        owner_device = chosen // CAP
        item_row = jax.random.randint(key_row, (impressions,), 0, ITEM_DEV)
        return (owner_device * ITEM_DEV + item_row).astype(jnp.int32)
    return jax.vmap(per_device)(jax.random.split(key, DEVICES)).reshape(USERS, CAND)


def make_table(key):
    return jax.random.truncated_normal(key, -6.0, 6.0, (ITEMS, 2 * D), jnp.float32)


def draw_candidates(key, part):
    return pick_candidates(jax.random.fold_in(key, 11))


def draw_item_table(key, part):
    return make_table(jax.random.fold_in(key, 12)).astype(jnp.bfloat16)


def draw_lengths(key, part):
    level_key, length_key = jax.random.split(jax.random.fold_in(key, 21))
    levels = jax.random.randint(level_key, (DEVICES, 1), 0, 4)
    highest = jnp.maximum(jnp.right_shift(jnp.full((DEVICES, 1), MAXB * BLK, jnp.int32), levels), BLK // 8 + 1)
    drawn = jax.random.randint(length_key, (DEVICES, U_DEV), BLK // 8, highest + 1)
    drawn = drawn.at[0, 0].set(MAXB * BLK).at[0, 1].set(BLK // 8)
    return drawn.reshape(USERS).astype(jnp.int32)


def draw_history(key, part):
    base_key = jax.random.fold_in(key, 13)
    return jax.random.truncated_normal(base_key, -6.0, 6.0, (USERS, MAXB * BLK, D), jnp.float32).astype(jnp.bfloat16)


def gaussian(own_key, extent, deviation, most, kind=jnp.bfloat16):
    values = jax.random.normal(own_key, extent, jnp.float32) * deviation
    return jnp.minimum(jnp.maximum(values, -most), most).astype(kind)


def setup_inputs(seed: int = 0) -> dict:
    seeds = jax.random.split(jax.random.key(seed), 10)
    return {
        "history": draw_history(jax.random.fold_in(seeds[9], 71), 0),
        "lengths": draw_lengths(jax.random.fold_in(seeds[9], 71), 0),
        "candidates": draw_candidates(jax.random.fold_in(seeds[9], 71), 0),
        "item_table": draw_item_table(jax.random.fold_in(seeds[9], 71), 0),
        "value_weight": gaussian(seeds[4], (D, D), D ** -0.5, 0.375),
        "click_hidden": gaussian(seeds[5], (3 * D, TH), (3 * D) ** -0.5, 0.21875),
        "convert_hidden": gaussian(seeds[6], (3 * D, TH), (3 * D) ** -0.5, 0.21875),
        "click_output": gaussian(seeds[7], (TH,), (TH // 4) ** -0.5, 0.75),
        "convert_output": gaussian(seeds[8], (TH,), (TH // 4) ** -0.5, 0.75),
    }


def reference(history, lengths, candidates, item_table, value_weight, click_hidden, convert_hidden, click_output, convert_output):
    scale_factor = 1.0 / math.sqrt(HEAD_DIM)
    candidate_rows = item_table[candidates]
    target = candidate_rows[:, :, :D]
    features = candidate_rows[:, :, D:]
    value_heads = value_weight.astype(jnp.float32).reshape(D, HEADS, HEAD_DIM)

    def one_user(user_args):
        user_history, user_length, user_target = user_args
        blocks = user_history.reshape(MAXB, BLK, D).astype(jnp.float32)
        block_heads = blocks.reshape(MAXB, BLK, HEADS, HEAD_DIM)
        query = user_target.astype(jnp.float32).reshape(CAND, HEADS, HEAD_DIM)
        scores = jnp.einsum('chj,bthj->bcht', query, block_heads) * scale_factor
        place = jnp.arange(MAXB, dtype=jnp.int32)[:, None] * BLK + jnp.arange(BLK, dtype=jnp.int32)[None, :]
        live_key = (place < user_length)[:, None, None, :]
        masked = jnp.where(live_key, scores, -1e+30)
        block_max = lax.optimization_barrier(jnp.max(masked, -1))
        weights = jnp.where(live_key, jnp.exp(masked - block_max[..., None]), 0.0).astype(jnp.bfloat16)
        block_sum = lax.optimization_barrier(jnp.sum(weights.astype(jnp.float32), -1))
        block_context = jnp.einsum('bcht,btd->bchd', weights.astype(jnp.float32), blocks)
        top_max = lax.optimization_barrier(jnp.max(block_max, 0))
        factor = jnp.exp(block_max - top_max)
        total = lax.optimization_barrier(jnp.sum(factor * block_sum, 0))
        context = lax.optimization_barrier(jnp.sum(factor[..., None] * block_context, 0))
        numerator = jnp.einsum('chd,dhk->chk', context, value_heads, precision=lax.Precision.HIGHEST)
        pooled = (numerator / total[..., None]).reshape(CAND, D)
        normed = pooled * lax.rsqrt(lax.optimization_barrier(jnp.mean(pooled * pooled, -1, keepdims=True)) + 1e-06)
        return normed.astype(jnp.bfloat16)
    interest = lax.map(one_user, (history, lengths, target))
    joined = jnp.concatenate([interest, target, features], -1).reshape(USERS * CAND, 3 * D)
    click_act = jax.nn.relu(jnp.dot(joined, click_hidden, preferred_element_type=jnp.float32)).astype(jnp.bfloat16)
    convert_act = jax.nn.relu(jnp.dot(joined, convert_hidden, preferred_element_type=jnp.float32)).astype(jnp.bfloat16)
    click_rate = jax.nn.sigmoid(jnp.dot(click_act, click_output, preferred_element_type=jnp.float32))
    convert_rate = jax.nn.sigmoid(jnp.dot(convert_act, convert_output, preferred_element_type=jnp.float32))
    return (click_rate.reshape(USERS, CAND), (click_rate * convert_rate).reshape(USERS, CAND))
```

```python
import functools
import math

import jax
import jax.numpy as jnp
from jax import lax
from jax.experimental import pallas as pl
from jax.experimental.pallas import tpu as pltpu
from jax.sharding import PartitionSpec as P

HEADS = 4
CHUNK = 512
SPLIT = 256
MESH = pl.DeviceIdType.MESH
neg_big = -1e30
f32, bf16 = jnp.float32, jnp.bfloat16


def dot(a, b, dims=((1,), (0,))):
    return lax.dot_general(a, b, (dims, ((), ())), preferred_element_type=f32)


def iota(shape, axis):
    return lax.broadcasted_iota(jnp.int32, shape, axis)


def fused_kernel(
    n,
    ny,
    cap,
    cand_hbm,
    len_hbm,
    click_out_hbm,
    convert_out_hbm,
    table_hbm,
    hist_hbm,
    value_hbm,
    click_hbm,
    convert_hbm,
    logit_ref,
    cand_ref,
    len_ref,
    click_out_ref,
    convert_out_ref,
    table,
    hist,
    value,
    click,
    convert,
    id_send,
    id_recv,
    pick,
    target_send,
    target_recv,
    feature_send,
    feature_recv,
    scores,
    weights,
    keyed,
    hidden_t,
    partial,
    interest_t,
    load_sems,
    sems,
):
    me = lax.axis_index("gx") * ny + lax.axis_index("gy")
    users, per_user = cand_ref.shape
    seq, width = hist.shape[1:]
    total = users * per_user
    table_rows = table.shape[0]
    plane = n // 4
    me_z = lax.div(me, plane)
    me_r = lax.rem(me, plane)
    half = lax.div(me_z, 2)
    planes = (3 - 3 * half, 2 - half, 2 * half + 1 - lax.rem(me_z, 2), me_z)

    def at(q, k):
        d = planes[q] * plane + lax.rem(me_r + k, plane)
        return d, (lax.div(d, ny), lax.rem(d, ny))

    def each(lo, hi, body):
        for q in range(4):
            first, last = max(lo - q * plane, q // 3), min(hi - q * plane, plane)
            if first < last:
                lax.fori_loop(first, last, functools.partial(body, q), 0)

    barrier = pltpu.get_barrier_semaphore()

    def greet(q, k, c):
        pl.semaphore_signal(barrier, inc=1, device_id=at(q, k)[1], device_id_type=MESH)
        return c

    loads = [
        pltpu.make_async_copy(src, dst, load_sems.at[i])
        for i, (src, dst) in enumerate(
            [
                (cand_hbm, cand_ref),
                (table_hbm, table),
                (len_hbm, len_ref),
                (click_out_hbm, click_out_ref),
                (convert_out_hbm, convert_out_ref),
                (value_hbm, value),
                (click_hbm, click),
                (convert_hbm, convert),
            ]
            + [(hist_hbm.at[u], hist.at[u]) for u in range(users)]
        )
    ]
    loads[0].start()
    each(0, n, greet)
    for load in loads[1:]:
        load.start()
    loads[0].wait()

    ids = jnp.concatenate([cand_ref[u : u + 1, :] for u in range(users)], axis=1)
    first = iota((n, total), 0) * table_rows
    local = ids - first
    mine = (local >= 0) & (local < table_rows)
    hot = jnp.where(mine, 1.0, 0.0).astype(f32)
    earlier = jnp.where(iota((total, total), 0) < iota((total, total), 1), 1.0, 0.0).astype(bf16)
    rank = jnp.sum(hot * dot(hot.astype(bf16), earlier), axis=0, keepdims=True)
    owner = jnp.sum(hot * iota((n, total), 0).astype(f32), axis=0, keepdims=True)
    slot = owner * cap + rank
    high = jnp.where(mine, local // SPLIT, 0).astype(f32).astype(bf16)
    low = jnp.where(mine, local % SPLIT, 0).astype(f32).astype(bf16)
    rank_i = rank.astype(jnp.int32)
    lane = iota((128, total), 0)
    at_high = jnp.where(lane == rank_i, 1.0, 0.0).astype(bf16)
    at_low = jnp.where(lane == rank_i + cap, 1.0, 0.0).astype(bf16)
    request = dot(high, at_high, ((1,), (1,))) + dot(low, at_low, ((1,), (1,)))
    for d in range(n):
        id_send[d] = request[d : d + 1, :]

    def send(src, dst, lo, hi, sem, by_owner):
        def one(q, k, c):
            d, where = at(q, k)
            pltpu.make_async_remote_copy(
                src_ref=src.at[d if by_owner else q * plane + k],
                dst_ref=dst.at[me],
                send_sem=sems.at[sem],
                recv_sem=sems.at[sem + 1],
                device_id=where,
                device_id_type=MESH,
            ).start()
            return c

        each(lo, hi, one)

    others = pl.ds(0, n - 1)

    def drain(ref, sem):
        pltpu.make_async_copy(ref.at[others], ref.at[others], sems.at[sem]).wait()

    pl.semaphore_wait(barrier, n - 1)
    send(id_send, id_recv, 0, n, 0, True)
    id_recv[me] = id_send[me]

    same = iota((total, total), 0) == iota((total, total), 1)
    slot_col = jnp.sum(jnp.where(same, slot, 0.0), axis=1, keepdims=True).astype(jnp.int32)
    choose = jnp.where(slot_col == iota((total, n * cap), 1), 1.0, 0.0).astype(bf16)

    drain(id_recv, 1)
    group = 256 // cap
    asked = jnp.concatenate([id_recv[d] for d in range(n)], axis=0).astype(bf16)
    loads[1].wait()
    for g in range(n // group):
        base = g * group
        turn = base + iota((256, n), 0) // cap
        quarter = turn // plane
        source = jnp.where(quarter == 0, planes[0], planes[3])
        source = jnp.where(quarter == 1, planes[1], jnp.where(quarter == 2, planes[2], source))
        source = source * plane + lax.rem(me_r + turn % plane, plane)
        expand = jnp.where(source == iota((256, n), 1), 1.0, 0.0).astype(bf16)
        spread = dot(expand, asked)
        place = iota((256, 128), 0) % cap
        lane = iota((256, 128), 1)
        weight = jnp.where(lane == place, float(SPLIT), jnp.where(lane == place + cap, 1.0, 0.0))
        wanted = jnp.sum(spread * weight, axis=1, keepdims=True).astype(jnp.int32)
        pick[g] = jnp.where(wanted == iota((256, table_rows), 1), 1.0, 0.0).astype(bf16)
        found = dot(pick[g], table[:, :width]).astype(bf16)
        for k in range(group):
            target_send[base + k] = found[k * cap : (k + 1) * cap, :]
        send(target_send, target_recv, base, base + group, 2, False)
    for g in range(n // group):
        base = g * group
        found = dot(pick[g], table[:, width:]).astype(bf16)
        for k in range(group):
            feature_send[base + k] = found[k * cap : (k + 1) * cap, :]
        send(feature_send, feature_recv, base, base + group, 4, False)
    target_recv[me] = target_send[3 * plane]
    feature_recv[me] = feature_send[3 * plane]

    for load in loads[2:]:
        load.wait()
    head = width // HEADS
    queries = HEADS * per_user
    scale = math.log2(math.e) / math.sqrt(head)
    hide = click.shape[1]
    same = iota((width, width), 0) == iota((width, width), 1)
    eye = jnp.where(same, 1.0, 0.0).astype(bf16)

    def turned(x):
        return dot(eye, x, ((1,), (1,))).astype(bf16)

    hidden_t[:hide, :] = turned(click[...])
    hidden_t[hide:, :] = turned(convert[...])
    value_t = turned(value[...])
    for u in range(users):
        first_row = hist[u, :1, :].astype(f32)
        for c in range(seq // CHUNK):
            rows = slice(c * CHUNK, (c + 1) * CHUNK)
            own = hist[u, rows, :]
            made = dot(value_t, own, ((1,), (1,)))
            live = iota((1, CHUNK), 1) < len_ref[u] - c * CHUNK
            keyed[u, :width, rows] = jnp.where(live, made, 0.0).astype(bf16)
            keyed[u, width:, rows] = jnp.where(
                iota((16, CHUNK), 1) < len_ref[u] - c * CHUNK, 1.0, 0.0
            ).astype(bf16)
            live_row = iota((CHUNK, 1), 0) < len_ref[u] - c * CHUNK
            hist[u, rows, :] = jnp.where(live_row, own.astype(f32), first_row).astype(bf16)

    drain(target_recv, 3)
    target = dot(choose, target_recv[...].reshape(n * cap, width)).astype(bf16)
    lane_head = iota((per_user, width), 1) // head

    def query_of(u):
        own = target[u * per_user : (u + 1) * per_user, :]
        return jnp.concatenate(
            [jnp.where(lane_head == h, own, jnp.zeros_like(own)) for h in range(HEADS)], axis=0
        )

    def score(u, c, query, top):
        rows = slice(c * CHUNK, (c + 1) * CHUNK)
        s = dot(hist[u, rows, :], query, ((1,), (1,)))
        scores[u % 2, rows, :] = s
        part = jnp.max(s.reshape(CHUNK // 8, 8, queries), axis=0)
        return part if top is None else jnp.maximum(top, part)

    def weigh(u, c, top):
        rows = slice(c * CHUNK, (c + 1) * CHUNK)
        w = jnp.exp2((scores[u % 2, rows, :] - top) * scale).astype(bf16)
        weights[u % 2, rows, :] = w

    pooled = []

    def interest(u):
        context = dot(keyed[u], weights[u % 2])
        inverse = 1.0 / context[width : width + 1, :]
        parts = []
        for h in range(HEADS):
            tile = slice(h // 2 * 2 * head, (h // 2 + 1) * 2 * head)
            part = context[h * head : (h + 1) * head, tile] * inverse[:, tile]
            parts.append(part if h % 2 == u % 2 else pltpu.roll(part, head, 1))
        raw = jnp.concatenate(parts, axis=0)
        normed = raw * lax.rsqrt(jnp.mean(raw * raw, axis=0, keepdims=True) + 1e-6)
        if u % 2 == 0:
            pooled.append(normed)
        else:
            left = iota((width, 2 * head), 1) < head
            both = jnp.where(left, pooled.pop(), normed)
            interest_t[:, (u - 1) * per_user : (u + 1) * per_user] = both.astype(bf16)

    query = query_of(0)
    top = None
    for c in range(seq // CHUNK):
        top = score(0, c, query, top)
    partial[...] = dot(hidden_t[:, width : 2 * width], target, ((1,), (1,)))
    for u in range(users):
        now = jnp.max(top, axis=0, keepdims=True)
        top = None
        if u + 1 < users:
            query = query_of(u + 1)
        for c in range(seq // CHUNK):
            if u + 1 < users:
                top = score(u + 1, c, query, top)
            weigh(u, c, now)
        interest(u)
    partial[...] += dot(hidden_t[:, :width], interest_t[...])

    drain(feature_recv, 5)
    feature = dot(choose, feature_recv[...].reshape(n * cap, width)).astype(bf16)
    act = partial[...] + dot(hidden_t[:, 2 * width :], feature, ((1,), (1,)))
    act = jnp.maximum(act, 0.0).astype(bf16)
    for i, output_ref in enumerate([click_out_ref, convert_out_ref]):
        logit = dot(output_ref[...].reshape(1, -1), act[i * hide : (i + 1) * hide, :])
        for u in range(users):
            logit_ref[i, u : u + 1, :] = logit[:, u * per_user : (u + 1) * per_user]
    drain(id_send, 0)
    drain(target_send, 2)
    drain(feature_send, 4)


def local(
    n,
    ny,
    history,
    lengths,
    candidates,
    item_table,
    value_weight,
    click_hidden,
    convert_hidden,
    click_output,
    convert_output,
):
    users, per_user = candidates.shape
    seq, width = history.shape[1:]
    total = users * per_user
    cap = max(2 * total // n, 16)
    queries = HEADS * per_user
    slab = pltpu.VMEM((n, cap, width), bf16)
    held = [click_output, convert_output, item_table, history, value_weight, click_hidden, convert_hidden]
    logits = pl.pallas_call(
        functools.partial(fused_kernel, n, ny, cap),
        out_shape=pltpu.VMEM((2, users, per_user), f32),
        in_specs=[pl.BlockSpec(memory_space=pl.ANY)] * 9,
        out_specs=pl.BlockSpec(memory_space=pltpu.VMEM),
        scratch_shapes=[pltpu.VMEM(candidates.shape, jnp.int32), pltpu.SMEM(lengths.shape, jnp.int32)]
        + [pltpu.VMEM(x.shape, x.dtype) for x in held]
        + [
            pltpu.VMEM((n, 1, 128), f32),
            pltpu.VMEM((n, 1, 128), f32),
            pltpu.VMEM((n * cap // 256, 256, item_table.shape[0]), bf16),
            slab,
            slab,
            slab,
            slab,
            pltpu.VMEM((2, seq, queries), f32),
            pltpu.VMEM((2, seq, queries), bf16),
            pltpu.VMEM((users, width + 16, seq), bf16),
            pltpu.VMEM((2 * click_hidden.shape[1], 3 * width), bf16),
            pltpu.VMEM((2 * click_hidden.shape[1], total), f32),
            pltpu.VMEM((width, total), bf16),
            pltpu.SemaphoreType.DMA((8 + users,)),
            pltpu.SemaphoreType.DMA((6,)),
        ],
        compiler_params=pltpu.CompilerParams(collective_id=0, has_side_effects=True),
        name="esmm",
    )(candidates, lengths, *held)
    rate = 1.0 / (1.0 + jnp.exp(-logits[0]))
    return rate, rate / (1.0 + jnp.exp(-logits[1]))


def solution(mesh):
    both = ("gx", "gy")
    placed = (P(both, None, None), P(both), P(both, None), P(both, None), P(), P(), P(), P(), P())
    return jax.shard_map(
        functools.partial(local, mesh.shape["gx"] * mesh.shape["gy"], mesh.shape["gy"]),
        mesh=mesh,
        in_specs=placed,
        out_specs=(P(both, None), P(both, None)),
        check_vma=False,
    )
```

```python
import functools
import math

import jax
import jax.numpy as jnp
from jax import lax
from jax.experimental import pallas as pl
from jax.experimental.pallas import tpu as pltpu
from jax.sharding import PartitionSpec as P

HEADS = 4
CHUNK = 512
SPLIT = 256
SHARE = 128
MESH = pl.DeviceIdType.MESH
neg_big = -1e30
f32, bf16 = jnp.float32, jnp.bfloat16


def dot(a, b, dims=((1,), (0,))):
    return lax.dot_general(a, b, (dims, ((), ())), preferred_element_type=f32)


def iota(shape, axis):
    return lax.broadcasted_iota(jnp.int32, shape, axis)


def fused_kernel(
    n,
    ny,
    cap,
    cand_hbm,
    len_hbm,
    click_out_hbm,
    convert_out_hbm,
    table_hbm,
    hist_hbm,
    value_hbm,
    click_hbm,
    convert_hbm,
    logit_ref,
    cand_ref,
    len_ref,
    click_out_ref,
    convert_out_ref,
    table,
    hist,
    value,
    click,
    convert,
    id_send,
    id_recv,
    pick,
    target_send,
    target_recv,
    feature_send,
    feature_recv,
    scores,
    weights,
    keyed,
    hidden_t,
    partial,
    interest_t,
    load_sems,
    sems,
    id_sems,
    late_sem,
):
    me = lax.axis_index("gx") * ny + lax.axis_index("gy")
    users, per_user = cand_ref.shape
    seq, width = hist.shape[1:]
    total = users * per_user
    table_rows = table.shape[0]
    plane = n // 4
    me_z = lax.div(me, plane)
    me_r = lax.rem(me, plane)
    half = lax.div(me_z, 2)
    planes = (3 - 3 * half, 2 - half, 2 * half + 1 - lax.rem(me_z, 2), me_z)

    def at(q, k, turn=True):
        r = lax.rem(me_r + k, plane) if turn else k
        d = planes[q] * plane + r
        return d, q * plane + r, (lax.div(d, ny), lax.rem(d, ny))

    def each(q, body):
        lax.fori_loop(q // 3, plane, functools.partial(body, q), 0)

    barrier = pltpu.get_barrier_semaphore()

    def greet(sem, q, k, c):
        pl.semaphore_signal(sem, inc=1, device_id=at(q, k)[2], device_id_type=MESH)
        return c

    loads = [
        pltpu.make_async_copy(src, dst, load_sems.at[i])
        for i, (src, dst) in enumerate(
            [
                (cand_hbm, cand_ref),
                (table_hbm, table),
                (len_hbm, len_ref),
                (click_out_hbm, click_out_ref),
                (convert_out_hbm, convert_out_ref),
                (value_hbm, value),
                (click_hbm, click),
                (convert_hbm, convert),
            ]
            + [(hist_hbm.at[u], hist.at[u]) for u in range(users)]
        )
    ]
    loads[0].start()
    last = me_z == 3

    @pl.when(jnp.logical_not(last))
    def _():
        for q in range(3):
            each(q, functools.partial(greet, barrier))

    each(3, functools.partial(greet, barrier))
    for load in loads[1:]:
        load.start()

    @pl.when(last)
    def _():
        pl.semaphore_wait(barrier, n - 1)
        for q in range(3):
            each(q, functools.partial(greet, late_sem))

    loads[0].wait()

    ids = jnp.concatenate([cand_ref[u : u + 1, :] for u in range(users)], axis=1)
    first = iota((n, total), 0) * table_rows
    local = ids - first
    mine = (local >= 0) & (local < table_rows)
    hot = jnp.where(mine, 1.0, 0.0).astype(f32)
    earlier = jnp.where(iota((total, total), 0) < iota((total, total), 1), 1.0, 0.0).astype(bf16)
    rank = jnp.sum(hot * dot(hot.astype(bf16), earlier), axis=0, keepdims=True)
    owner = jnp.sum(hot * iota((n, total), 0).astype(f32), axis=0, keepdims=True)
    slot = owner * cap + rank
    high = jnp.where(mine, local // SPLIT, 0).astype(f32).astype(bf16)
    low = jnp.where(mine, local % SPLIT, 0).astype(f32).astype(bf16)
    at_rank = jnp.where(iota((128, total), 0) == rank.astype(jnp.int32), 1.0, 0.0).astype(bf16)
    request = SPLIT * dot(high, at_rank, ((1,), (1,))) + dot(low, at_rank, ((1,), (1,)))
    for d in range(n):
        id_send[d] = request[d : d + 1, :]

    def copy_to(where, src, dst, send_sem, recv_sem):
        pltpu.make_async_remote_copy(
            src_ref=src,
            dst_ref=dst,
            send_sem=send_sem,
            recv_sem=recv_sem,
            device_id=where,
            device_id_type=MESH,
        ).start()

    def send_ids(q, k, c):
        d, _, where = at(q, k)
        copy_to(where, id_send.at[d], id_recv.at[me], sems.at[0], id_sems.at[me_z])
        return c

    def send_rows(src, dst, sem, turn, q, k, c):
        _, place, where = at(q, k, turn)
        copy_to(where, src.at[place], dst.at[me], sems.at[sem], sems.at[sem + 1])
        return c

    def drain(ref, sem, count=n - 1):
        some = ref.at[pl.ds(0, count)]
        pltpu.make_async_copy(some, some, sem).wait()

    @pl.when(last)
    def _():
        for q in range(3):
            each(q, send_ids)

    @pl.when(jnp.logical_not(last))
    def _():
        pl.semaphore_wait(barrier, n - 1 - plane)

        @pl.when(half == 0)
        def _():
            each(1, send_ids)
            each(2, send_ids)
            pl.semaphore_wait(late_sem, plane)
            each(0, send_ids)

        @pl.when(half == 1)
        def _():
            each(0, send_ids)
            each(1, send_ids)
            pl.semaphore_wait(late_sem, plane)
            each(2, send_ids)

    each(3, send_ids)
    id_recv[me] = id_send[me]

    same = iota((total, total), 0) == iota((total, total), 1)
    slot_col = jnp.sum(jnp.where(same, slot, 0.0), axis=1, keepdims=True).astype(jnp.int32)
    choose = jnp.where(slot_col == iota((total, n * cap), 1), 1.0, 0.0).astype(bf16)

    def gather(qs, part, dst):
        steps = [(q, i) for q in qs for i in range(plane * cap // SHARE)]
        many = 256 // SHARE
        for j in range(0, len(steps), many):
            some = steps[j : j + many]
            picks, places = [], []
            for q, i in some:
                base = q * plane + i * (SHARE // cap)
                at_rows = slice(base * cap, base * cap + SHARE)
                if part == 0:
                    asked = id_recv[pl.ds(planes[q] * plane + i * (SHARE // cap), SHARE // cap)]
                    spread = jnp.broadcast_to(asked, (SHARE // cap, cap, 128)).reshape(SHARE, 128)
                    place = iota((SHARE, 128), 0) % cap == iota((SHARE, 128), 1)
                    wanted = jnp.sum(jnp.where(place, spread, 0.0), axis=1, keepdims=True).astype(jnp.int32)
                    pick[at_rows, :] = jnp.where(wanted == iota((SHARE, table_rows), 1), 1.0, 0.0).astype(bf16)
                picks.append(pick[at_rows, :])
                places += [base + k for k in range(SHARE // cap)]
            found = dot(jnp.concatenate(picks, axis=0), table[:, part * width : (part + 1) * width]).astype(bf16)
            for k, at_slot in enumerate(places):
                dst[at_slot] = found[k * cap : (k + 1) * cap, :]

    loads[1].wait()
    for qs in ((1,), (0,), (2, 3)):
        for q in qs:
            drain(id_recv, id_sems.at[planes[q]], plane - q // 3)
        gather(qs, 0, target_send)
        for q in qs:
            each(q, functools.partial(send_rows, target_send, target_recv, 2, q > 0))
    for load in loads[2:]:
        load.wait()
    head = width // HEADS
    queries = HEADS * per_user
    scale = math.log2(math.e) / math.sqrt(head)
    hide = click.shape[1]
    same = iota((width, width), 0) == iota((width, width), 1)
    eye = jnp.where(same, 1.0, 0.0).astype(bf16)

    def turned(x):
        return dot(eye, x, ((1,), (1,))).astype(bf16)

    hidden_t[:hide, :] = turned(click[...])
    hidden_t[hide:, :] = turned(convert[...])
    value_t = turned(value[...])
    def prepare(u):
        first_row = hist[u, :1, :].astype(f32)
        for c in range(seq // CHUNK):
            rows = slice(c * CHUNK, (c + 1) * CHUNK)
            own = hist[u, rows, :]
            made = dot(value_t, own, ((1,), (1,)))
            live = iota((1, CHUNK), 1) < len_ref[u] - c * CHUNK
            keyed[u, :width, rows] = jnp.where(live, made, 0.0).astype(bf16)
            keyed[u, width:, rows] = jnp.where(
                iota((16, CHUNK), 1) < len_ref[u] - c * CHUNK, 1.0, 0.0
            ).astype(bf16)
            live_row = iota((CHUNK, 1), 0) < len_ref[u] - c * CHUNK
            hist[u, rows, :] = jnp.where(live_row, own.astype(f32), first_row).astype(bf16)

    for u in range(2):
        prepare(u)
    for qs in ((0, 1), (2, 3)):
        gather(qs, 1, feature_send)
        for q in qs:
            each(q, functools.partial(send_rows, feature_send, feature_recv, 4, q > 0))
    for u in range(2, users):
        prepare(u)
    target_recv[me] = target_send[3 * plane + me_r]
    feature_recv[me] = feature_send[3 * plane + me_r]

    drain(target_recv, sems.at[3])
    target = dot(choose, target_recv[...].reshape(n * cap, width)).astype(bf16)
    lane_head = iota((per_user, width), 1) // head

    def query_of(u):
        own = target[u * per_user : (u + 1) * per_user, :]
        return jnp.concatenate(
            [jnp.where(lane_head == h, own, jnp.zeros_like(own)) for h in range(HEADS)], axis=0
        )

    def score(u, c, query, top):
        rows = slice(c * CHUNK, (c + 1) * CHUNK)
        s = dot(hist[u, rows, :], query, ((1,), (1,)))
        scores[u % 2, rows, :] = s
        part = jnp.max(s.reshape(CHUNK // 8, 8, queries), axis=0)
        return part if top is None else jnp.maximum(top, part)

    def weigh(u, c, top):
        rows = slice(c * CHUNK, (c + 1) * CHUNK)
        w = jnp.exp2((scores[u % 2, rows, :] - top) * scale).astype(bf16)
        weights[u % 2, rows, :] = w

    pooled = []

    def interest(u):
        context = dot(keyed[u], weights[u % 2])
        inverse = 1.0 / context[width : width + 1, :]
        parts = []
        for h in range(HEADS):
            tile = slice(h // 2 * 2 * head, (h // 2 + 1) * 2 * head)
            part = context[h * head : (h + 1) * head, tile] * inverse[:, tile]
            parts.append(part if h % 2 == u % 2 else pltpu.roll(part, head, 1))
        raw = jnp.concatenate(parts, axis=0)
        normed = raw * lax.rsqrt(jnp.mean(raw * raw, axis=0, keepdims=True) + 1e-6)
        if u % 2 == 0:
            pooled.append(normed)
        else:
            left = iota((width, 2 * head), 1) < head
            both = jnp.where(left, pooled.pop(), normed)
            interest_t[:, (u - 1) * per_user : (u + 1) * per_user] = both.astype(bf16)

    query = query_of(0)
    top = None
    for c in range(seq // CHUNK):
        top = score(0, c, query, top)
    partial[...] = dot(hidden_t[:, width : 2 * width], target, ((1,), (1,)))
    for u in range(users):
        now = jnp.max(top, axis=0, keepdims=True)
        top = None
        if u + 1 < users:
            query = query_of(u + 1)
        for c in range(seq // CHUNK):
            if u + 1 < users:
                top = score(u + 1, c, query, top)
            weigh(u, c, now)
        interest(u)
    partial[...] += dot(hidden_t[:, :width], interest_t[...])

    drain(feature_recv, sems.at[5])
    feature = dot(choose, feature_recv[...].reshape(n * cap, width)).astype(bf16)
    act = partial[...] + dot(hidden_t[:, 2 * width :], feature, ((1,), (1,)))
    act = jnp.maximum(act, 0.0).astype(bf16)
    for i, output_ref in enumerate([click_out_ref, convert_out_ref]):
        logit = dot(output_ref[...].reshape(1, -1), act[i * hide : (i + 1) * hide, :])
        for u in range(users):
            logit_ref[i, u : u + 1, :] = logit[:, u * per_user : (u + 1) * per_user]
    drain(id_send, sems.at[0])
    drain(target_send, sems.at[2])
    drain(feature_send, sems.at[4])


def local(
    n,
    ny,
    history,
    lengths,
    candidates,
    item_table,
    value_weight,
    click_hidden,
    convert_hidden,
    click_output,
    convert_output,
):
    users, per_user = candidates.shape
    seq, width = history.shape[1:]
    total = users * per_user
    cap = max(2 * total // n, 16)
    queries = HEADS * per_user
    slab = pltpu.VMEM((n, cap, width), bf16)
    held = [click_output, convert_output, item_table, history, value_weight, click_hidden, convert_hidden]
    logits = pl.pallas_call(
        functools.partial(fused_kernel, n, ny, cap),
        out_shape=pltpu.VMEM((2, users, per_user), f32),
        in_specs=[pl.BlockSpec(memory_space=pl.ANY)] * 9,
        out_specs=pl.BlockSpec(memory_space=pltpu.VMEM),
        scratch_shapes=[pltpu.VMEM(candidates.shape, jnp.int32), pltpu.SMEM(lengths.shape, jnp.int32)]
        + [pltpu.VMEM(x.shape, x.dtype) for x in held]
        + [
            pltpu.VMEM((n, 1, 128), f32),
            pltpu.VMEM((n, 1, 128), f32),
            pltpu.VMEM((n * cap, item_table.shape[0]), bf16),
            slab,
            slab,
            slab,
            slab,
            pltpu.VMEM((2, seq, queries), f32),
            pltpu.VMEM((2, seq, queries), bf16),
            pltpu.VMEM((users, width + 16, seq), bf16),
            pltpu.VMEM((2 * click_hidden.shape[1], 3 * width), bf16),
            pltpu.VMEM((2 * click_hidden.shape[1], total), f32),
            pltpu.VMEM((width, total), bf16),
            pltpu.SemaphoreType.DMA((8 + users,)),
            pltpu.SemaphoreType.DMA((6,)),
            pltpu.SemaphoreType.DMA((4,)),
            pltpu.SemaphoreType.REGULAR,
        ],
        compiler_params=pltpu.CompilerParams(collective_id=0, has_side_effects=True),
        name="esmm",
    )(candidates, lengths, *held)
    rate = 1.0 / (1.0 + jnp.exp(-logits[0]))
    return rate, rate / (1.0 + jnp.exp(-logits[1]))


def solution(mesh):
    both = ("gx", "gy")
    placed = (P(both, None, None), P(both), P(both, None), P(both, None), P(), P(), P(), P(), P())
    return jax.shard_map(
        functools.partial(local, mesh.shape["gx"] * mesh.shape["gy"], mesh.shape["gy"]),
        mesh=mesh,
        in_specs=placed,
        out_specs=(P(both, None), P(both, None)),
        check_vma=False,
    )
```

```python
import functools
import math

import jax
import jax.numpy as jnp
from jax import lax
from jax.experimental import pallas as pl
from jax.experimental.pallas import tpu as pltpu
from jax.sharding import PartitionSpec as P

HEADS = 4
CHUNK = 512
SPLIT = 256
SHARE = 128
TILE = 512
MESH = pl.DeviceIdType.MESH
neg_big = -1e30
f32, bf16 = jnp.float32, jnp.bfloat16


def dot(a, b, dims=((1,), (0,))):
    return lax.dot_general(a, b, (dims, ((), ())), preferred_element_type=f32)


def iota(shape, axis):
    return lax.broadcasted_iota(jnp.int32, shape, axis)


def fused_kernel(
    n,
    ny,
    cap,
    cand_hbm,
    len_hbm,
    click_out_hbm,
    convert_out_hbm,
    table_hbm,
    hist_hbm,
    value_hbm,
    click_hbm,
    convert_hbm,
    logit_ref,
    cand_ref,
    len_ref,
    click_out_ref,
    convert_out_ref,
    table,
    hist,
    value,
    click,
    convert,
    id_send,
    id_recv,
    pick,
    target_send,
    target_recv,
    feature_send,
    feature_recv,
    scores,
    weights,
    keyed,
    hidden_t,
    partial,
    interest_t,
    load_sems,
    sems,
    id_sems,
    late_sem,
):
    me = lax.axis_index("gx") * ny + lax.axis_index("gy")
    users, per_user = cand_ref.shape
    seq, width = hist.shape[1:]
    total = users * per_user
    table_rows = table.shape[0]
    plane = n // 4
    me_z = lax.div(me, plane)
    me_r = lax.rem(me, plane)
    half = lax.div(me_z, 2)
    planes = (3 - 3 * half, 2 - half, 2 * half + 1 - lax.rem(me_z, 2), me_z)

    def at(q, k, turn=True):
        r = lax.rem(me_r + k, plane) if turn else k
        d = planes[q] * plane + r
        return d, q * plane + r, (lax.div(d, ny), lax.rem(d, ny))

    def each(q, body):
        def eight(c, done):
            for k in range(8):
                body(q, c * 8 + k, 0)
            return done

        for k in range(q // 3, 8):
            body(q, k, 0)
        if plane > 8:
            lax.fori_loop(1, plane // 8, eight, 0)

    barrier = pltpu.get_barrier_semaphore()

    def greet(sem, q, k, c):
        pl.semaphore_signal(sem, inc=1, device_id=at(q, k)[2], device_id_type=MESH)
        return c

    loads = [
        pltpu.make_async_copy(src, dst, load_sems.at[i])
        for i, (src, dst) in enumerate(
            [
                (cand_hbm, cand_ref),
                (table_hbm, table),
                (len_hbm, len_ref),
                (click_out_hbm, click_out_ref),
                (convert_out_hbm, convert_out_ref),
                (value_hbm, value),
                (click_hbm, click),
                (convert_hbm, convert),
            ]
            + [(hist_hbm.at[u], hist.at[u]) for u in range(users)]
        )
    ]
    loads[0].start()
    last = me_z == 3

    @pl.when(jnp.logical_not(last))
    def _():
        for q in range(3):
            each(q, functools.partial(greet, barrier))

    each(3, functools.partial(greet, barrier))
    for load in loads[1:]:
        load.start()

    @pl.when(last)
    def _():
        pl.semaphore_wait(barrier, n - 1)
        for q in range(3):
            each(q, functools.partial(greet, late_sem))

    loads[0].wait()

    ids = jnp.concatenate([cand_ref[u : u + 1, :] for u in range(users)], axis=1)
    first = iota((n, total), 0) * table_rows
    local = ids - first
    mine = (local >= 0) & (local < table_rows)
    hot = jnp.where(mine, 1.0, 0.0).astype(f32)
    earlier = jnp.where(iota((total, total), 0) < iota((total, total), 1), 1.0, 0.0).astype(bf16)
    rank = jnp.sum(hot * dot(hot.astype(bf16), earlier), axis=0, keepdims=True)
    owner = jnp.sum(hot * iota((n, total), 0).astype(f32), axis=0, keepdims=True)
    slot = owner * cap + rank
    high = jnp.where(mine, local // SPLIT, 0).astype(f32).astype(bf16)
    low = jnp.where(mine, local % SPLIT, 0).astype(f32).astype(bf16)
    at_rank = jnp.where(iota((128, total), 0) == rank.astype(jnp.int32), 1.0, 0.0).astype(bf16)
    request = SPLIT * dot(high, at_rank, ((1,), (1,))) + dot(low, at_rank, ((1,), (1,)))
    for d in range(n):
        id_send[d] = request[d : d + 1, :]

    def copy_to(where, src, dst, send_sem, recv_sem):
        pltpu.make_async_remote_copy(
            src_ref=src,
            dst_ref=dst,
            send_sem=send_sem,
            recv_sem=recv_sem,
            device_id=where,
            device_id_type=MESH,
        ).start()

    def send_ids(q, k, c):
        d, _, where = at(q, k)
        copy_to(where, id_send.at[d], id_recv.at[me], sems.at[0], id_sems.at[me_z])
        return c

    def send_rows(src, dst, sem, turn, q, k, c):
        _, place, where = at(q, k, turn)
        copy_to(where, src.at[place], dst.at[me], sems.at[sem], sems.at[sem + 1])
        return c

    def drain(ref, sem, count=n - 1):
        some = ref.at[pl.ds(0, count)]
        pltpu.make_async_copy(some, some, sem).wait()

    @pl.when(last)
    def _():
        for q in range(3):
            each(q, send_ids)

    @pl.when(jnp.logical_not(last))
    def _():
        pl.semaphore_wait(barrier, n - 1 - plane)

        @pl.when(half == 0)
        def _():
            each(1, send_ids)
            each(2, send_ids)
            pl.semaphore_wait(late_sem, plane)
            each(0, send_ids)

        @pl.when(half == 1)
        def _():
            each(0, send_ids)
            each(1, send_ids)
            pl.semaphore_wait(late_sem, plane)
            each(2, send_ids)

    each(3, send_ids)
    id_recv[me] = id_send[me]

    same = iota((total, total), 0) == iota((total, total), 1)
    slot_col = jnp.sum(jnp.where(same, slot, 0.0), axis=1, keepdims=True).astype(jnp.int32)
    choose = jnp.where(slot_col == iota((total, n * cap), 1), 1.0, 0.0).astype(bf16)

    def gather(qs, part, dst):
        steps = [(q, i) for q in qs for i in range(plane * cap // SHARE)]
        many = 256 // SHARE
        for j in range(0, len(steps), many):
            some = steps[j : j + many]
            wanted, at_rows, places = [], [], []
            for q, i in some:
                base = q * plane + i * (SHARE // cap)
                at_rows.append(slice(base * cap, base * cap + SHARE))
                places += [base + k for k in range(SHARE // cap)]
                if part == 0:
                    asked = id_recv[pl.ds(planes[q] * plane + i * (SHARE // cap), SHARE // cap)]
                    spread = jnp.broadcast_to(asked, (SHARE // cap, cap, 128)).reshape(SHARE, 128)
                    place = iota((SHARE, 128), 0) % cap == iota((SHARE, 128), 1)
                    wanted.append(jnp.sum(jnp.where(place, spread, 0.0), axis=1, keepdims=True).astype(jnp.int32))
            found = None
            for t in range(table_rows // TILE):
                columns = slice(t * TILE, (t + 1) * TILE)
                picks = []
                for i, own in enumerate(at_rows):
                    if part == 0:
                        hit = wanted[i] - t * TILE == iota((SHARE, TILE), 1)
                        picks.append(jnp.where(hit, 1.0, 0.0).astype(bf16))
                        pick[own, columns] = picks[-1]
                    else:
                        picks.append(pick[own, columns])
                some_rows = table[columns, part * width : (part + 1) * width]
                more = dot(jnp.concatenate(picks, axis=0), some_rows)
                found = more if found is None else found + more
            found = found.astype(bf16)
            for k, at_slot in enumerate(places):
                dst[at_slot] = found[k * cap : (k + 1) * cap, :]

    loads[1].wait()
    for qs in ((1,), (0,), (2, 3)):
        for q in qs:
            drain(id_recv, id_sems.at[planes[q]], plane - q // 3)
        gather(qs, 0, target_send)
        for q in qs:
            each(q, functools.partial(send_rows, target_send, target_recv, 2, q > 0))
    for load in loads[2:]:
        load.wait()
    head = width // HEADS
    queries = HEADS * per_user
    scale = math.log2(math.e) / math.sqrt(head)
    hide = click.shape[1]
    same = iota((width, width), 0) == iota((width, width), 1)
    eye = jnp.where(same, 1.0, 0.0).astype(bf16)

    def turned(x):
        return dot(eye, x, ((1,), (1,))).astype(bf16)

    hidden_t[:hide, :] = turned(click[...])
    hidden_t[hide:, :] = turned(convert[...])
    value_t = turned(value[...])
    def prepare(u):
        first_row = hist[u, :1, :].astype(f32)
        for c in range(seq // CHUNK):
            rows = slice(c * CHUNK, (c + 1) * CHUNK)
            own = hist[u, rows, :]
            made = dot(value_t, own, ((1,), (1,)))
            live = iota((1, CHUNK), 1) < len_ref[u] - c * CHUNK
            keyed[u, :width, rows] = jnp.where(live, made, 0.0).astype(bf16)
            keyed[u, width:, rows] = jnp.where(
                iota((16, CHUNK), 1) < len_ref[u] - c * CHUNK, 1.0, 0.0
            ).astype(bf16)
            live_row = iota((CHUNK, 1), 0) < len_ref[u] - c * CHUNK
            hist[u, rows, :] = jnp.where(live_row, own.astype(f32), first_row).astype(bf16)

    for u in range(2):
        prepare(u)
    for qs in ((0, 1), (2, 3)):
        gather(qs, 1, feature_send)
        for q in qs:
            each(q, functools.partial(send_rows, feature_send, feature_recv, 4, q > 0))
    for u in range(2, users):
        prepare(u)
    target_recv[me] = target_send[3 * plane + me_r]
    feature_recv[me] = feature_send[3 * plane + me_r]

    drain(target_recv, sems.at[3])
    target = dot(choose, target_recv[...].reshape(n * cap, width)).astype(bf16)
    lane_head = iota((per_user, width), 1) // head

    def query_of(u):
        own = target[u * per_user : (u + 1) * per_user, :]
        return jnp.concatenate(
            [jnp.where(lane_head == h, own, jnp.zeros_like(own)) for h in range(HEADS)], axis=0
        )

    def score(u, c, query, top):
        rows = slice(c * CHUNK, (c + 1) * CHUNK)
        s = dot(hist[u, rows, :], query, ((1,), (1,)))
        scores[u % 2, rows, :] = s
        part = jnp.max(s.reshape(CHUNK // 8, 8, queries), axis=0)
        return part if top is None else jnp.maximum(top, part)

    def weigh(u, c, top):
        rows = slice(c * CHUNK, (c + 1) * CHUNK)
        w = jnp.exp2((scores[u % 2, rows, :] - top) * scale).astype(bf16)
        weights[u % 2, rows, :] = w

    pooled = []

    def interest(u):
        context = dot(keyed[u], weights[u % 2])
        inverse = 1.0 / context[width : width + 1, :]
        parts = []
        for h in range(HEADS):
            tile = slice(h // 2 * 2 * head, (h // 2 + 1) * 2 * head)
            part = context[h * head : (h + 1) * head, tile] * inverse[:, tile]
            parts.append(part if h % 2 == u % 2 else pltpu.roll(part, head, 1))
        raw = jnp.concatenate(parts, axis=0)
        normed = raw * lax.rsqrt(jnp.mean(raw * raw, axis=0, keepdims=True) + 1e-6)
        if u % 2 == 0:
            pooled.append(normed)
        else:
            left = iota((width, 2 * head), 1) < head
            both = jnp.where(left, pooled.pop(), normed)
            interest_t[:, (u - 1) * per_user : (u + 1) * per_user] = both.astype(bf16)

    query = query_of(0)
    top = None
    for c in range(seq // CHUNK):
        top = score(0, c, query, top)
    partial[...] = dot(hidden_t[:, width : 2 * width], target, ((1,), (1,)))
    for u in range(users):
        now = jnp.max(top, axis=0, keepdims=True)
        top = None
        if u + 1 < users:
            query = query_of(u + 1)
        for c in range(seq // CHUNK):
            if u + 1 < users:
                top = score(u + 1, c, query, top)
            weigh(u, c, now)
        interest(u)
    partial[...] += dot(hidden_t[:, :width], interest_t[...])

    ones = jnp.ones((total, total), bf16)
    out_rows = jnp.concatenate(
        [dot(jnp.where(same, ref[...].reshape(1, -1), 0.0).astype(bf16), ones) for ref in (click_out_ref, convert_out_ref)],
        axis=0,
    )
    drain(feature_recv, sems.at[5])
    feature = dot(choose, feature_recv[...].reshape(n * cap, width)).astype(bf16)
    act = partial[...] + dot(hidden_t[:, 2 * width :], feature, ((1,), (1,)))
    act = jnp.maximum(act, 0.0).astype(bf16)
    weighed = act.astype(f32) * out_rows
    for i in range(2):
        logit = jnp.sum(weighed[i * hide : (i + 1) * hide, :], axis=0, keepdims=True)
        for u in range(users):
            logit_ref[i, u : u + 1, :] = logit[:, u * per_user : (u + 1) * per_user]
    drain(id_send, sems.at[0])
    drain(target_send, sems.at[2])
    drain(feature_send, sems.at[4])


def local(
    n,
    ny,
    history,
    lengths,
    candidates,
    item_table,
    value_weight,
    click_hidden,
    convert_hidden,
    click_output,
    convert_output,
):
    users, per_user = candidates.shape
    seq, width = history.shape[1:]
    total = users * per_user
    cap = max(2 * total // n, 16)
    queries = HEADS * per_user
    slab = pltpu.VMEM((n, cap, width), bf16)
    held = [click_output, convert_output, item_table, history, value_weight, click_hidden, convert_hidden]
    logits = pl.pallas_call(
        functools.partial(fused_kernel, n, ny, cap),
        out_shape=pltpu.VMEM((2, users, per_user), f32),
        in_specs=[pl.BlockSpec(memory_space=pl.ANY)] * 9,
        out_specs=pl.BlockSpec(memory_space=pltpu.VMEM),
        scratch_shapes=[pltpu.VMEM(candidates.shape, jnp.int32), pltpu.SMEM(lengths.shape, jnp.int32)]
        + [pltpu.VMEM(x.shape, x.dtype) for x in held]
        + [
            pltpu.VMEM((n, 1, 128), f32),
            pltpu.VMEM((n, 1, 128), f32),
            pltpu.VMEM((n * cap, item_table.shape[0]), bf16),
            slab,
            slab,
            slab,
            slab,
            pltpu.VMEM((2, seq, queries), f32),
            pltpu.VMEM((2, seq, queries), bf16),
            pltpu.VMEM((users, width + 16, seq), bf16),
            pltpu.VMEM((2 * click_hidden.shape[1], 3 * width), bf16),
            pltpu.VMEM((2 * click_hidden.shape[1], total), f32),
            pltpu.VMEM((width, total), bf16),
            pltpu.SemaphoreType.DMA((8 + users,)),
            pltpu.SemaphoreType.DMA((6,)),
            pltpu.SemaphoreType.DMA((4,)),
            pltpu.SemaphoreType.REGULAR,
        ],
        compiler_params=pltpu.CompilerParams(collective_id=0, has_side_effects=True),
        name="esmm",
    )(candidates, lengths, *held)
    rate = 1.0 / (1.0 + jnp.exp(-logits[0]))
    return rate, rate / (1.0 + jnp.exp(-logits[1]))


def solution(mesh):
    both = ("gx", "gy")
    placed = (P(both, None, None), P(both), P(both, None), P(both, None), P(), P(), P(), P(), P())
    return jax.shard_map(
        functools.partial(local, mesh.shape["gx"] * mesh.shape["gy"], mesh.shape["gy"]),
        mesh=mesh,
        in_specs=placed,
        out_specs=(P(both, None), P(both, None)),
        check_vma=False,
    )
```
